128 devices in a mesh: dp: 1, ep: 128 (over z, y, x, core).
Axes of the slice: x: 4, y: 4, z: 4, core: 2. Of those that a mesh axis runs over, the one named last changes fastest.
Arguments:
- x_rows: bfloat16 [65536, 2048], P(('dp', 'ep'))
- logits: float32 [65536, 128], P(('dp', 'ep'))
- w_in: bfloat16 [128, 2048, 768], P('ep')
- w_out: bfloat16 [128, 768, 2048], P('ep')
Outputs:
- output: bfloat16 [65536, 2048], P(('dp', 'ep'))
All inputs are finite; a program needn't handle non-finite values.
Results may differ from the reference program's by a relative error of at most 0.001.
Values are sent between devices in bfloat16 or wider.
A program may use at most 1 GiB of HBM per device.

```python
import math
import jax
import jax.numpy as jnp
from jax import lax

TOKENS = 65536
D_MODEL = 2048
FF_HIDDEN = 768
EXPERTS = 128
CAPACITY = 1024
GROUP_DEV = 128
LOGIT_SHIFT = int(1024 * math.log(EXPERTS))


def draw_logits(route_key):
    sub_keys = jax.random.split(route_key, 5)
    tok_dev = TOKENS // GROUP_DEV
    mean_cnt = 2 * tok_dev // EXPERTS
    quarter = EXPERTS // 4
    exp_order = jax.random.permutation(sub_keys[0], EXPERTS)
    rot_bits = jax.random.randint(sub_keys[1], (GROUP_DEV,), 0, 2)
    tier_vals = jnp.array([2 * mean_cnt, mean_cnt, mean_cnt // 2, mean_cnt // 2], dtype=jnp.int32)
    tier_idx = (jnp.arange(EXPERTS)[None, :] // quarter + rot_bits[:, None]) % 4
    slot_ends = jnp.cumsum(tier_vals[tier_idx], axis=1)
    slot_ids = jnp.arange(2 * tok_dev)
    rank_pos = jnp.sum((slot_ends[:, None, :] <= slot_ids[None, :, None]).astype(jnp.int32), axis=2)
    pick_list = exp_order[rank_pos]
    perm_keys = jax.random.split(sub_keys[2], GROUP_DEV)
    tok_perm = jax.vmap(lambda perm_key: jax.random.permutation(perm_key, tok_dev))(perm_keys)
    first_pick = jnp.take_along_axis(pick_list[:, :tok_dev], tok_perm, axis=1).reshape(TOKENS)
    second_pick = jnp.take_along_axis(pick_list[:, tok_dev:], tok_perm, axis=1).reshape(TOKENS)
    expert_ids = jnp.arange(EXPERTS)
    chosen = (expert_ids[None, :] == first_pick[:, None]) | (expert_ids[None, :] == second_pick[:, None])
    base_val = jax.random.randint(sub_keys[3], (TOKENS, EXPERTS), 0, 2048)
    pick_val = jax.random.randint(sub_keys[4], (TOKENS, EXPERTS), 1024, 3072) + LOGIT_SHIFT
    score_int = jnp.where(chosen, pick_val, base_val) * EXPERTS + expert_ids[None, :]
    return score_int.astype(jnp.float32) / (1024.0 * EXPERTS)


def setup_inputs(seed: int = 0, part: int = 0) -> dict:
    part_key = jax.random.fold_in(jax.random.key(seed), part)
    sub_keys = jax.random.split(part_key, 2)
    w_keys = jax.random.split(jax.random.key(seed + 1), 2)
    x_rows = jax.random.normal(sub_keys[0], (TOKENS, D_MODEL), jnp.float32).astype(jnp.bfloat16)
    logits = draw_logits(sub_keys[1])
    w_in = (jax.random.normal(w_keys[0], (EXPERTS, D_MODEL, FF_HIDDEN), jnp.float32) * D_MODEL ** -0.5).astype(jnp.bfloat16)
    w_out = (jax.random.normal(w_keys[1], (EXPERTS, FF_HIDDEN, D_MODEL), jnp.float32) * (2.0 * FF_HIDDEN ** -0.5)).astype(jnp.bfloat16)
    return {'x_rows': x_rows, 'logits': logits, 'w_in': w_in, 'w_out': w_out}


def reference(x_rows, logits, w_in, w_out):
    gate_probs = jax.nn.softmax(logits, axis=-1)
    top_vals, top_ids = lax.top_k(logits, 2)
    chosen = (logits >= top_vals[:, 1:2]).astype(jnp.int32)
    before = jnp.cumsum(chosen, axis=0) - chosen
    pick_pos = jnp.take_along_axis(before, top_ids, axis=1)
    dest_row = jnp.where(pick_pos < CAPACITY, top_ids * CAPACITY + pick_pos, EXPERTS * CAPACITY)
    tok_ids = jnp.broadcast_to(jnp.arange(TOKENS, dtype=jnp.int32)[:, None], (TOKENS, 2))
    slot_tok = jnp.full((EXPERTS * CAPACITY,), TOKENS, jnp.int32).at[dest_row.reshape(-1)].set(tok_ids.reshape(-1), mode='drop')
    expert_rows = jnp.take(x_rows, slot_tok, axis=0, mode='fill', fill_value=0).reshape(EXPERTS, CAPACITY, D_MODEL)

    def expert_ffn(operands):
        rows_in, w_first, w_second = operands
        hidden = jax.nn.gelu(jnp.dot(rows_in, w_first, preferred_element_type=jnp.float32), approximate=True).astype(jnp.bfloat16)
        return jnp.dot(hidden, w_second, preferred_element_type=jnp.float32).astype(jnp.bfloat16)

    expert_out = lax.map(expert_ffn, (expert_rows, w_in, w_out)).reshape(EXPERTS * CAPACITY, D_MODEL)
    rows_back = jnp.take(expert_out, dest_row, axis=0, mode='fill', fill_value=0)
    pick_gate = jnp.take_along_axis(gate_probs, top_ids, axis=1)
    mix_sum = jnp.sum(pick_gate[:, :, None] * rows_back.astype(jnp.float32), axis=1)
    return (x_rows.astype(jnp.float32) + mix_sum).astype(jnp.bfloat16)
```

```python
import functools
import jax
import jax.numpy as jnp
from jax import lax
from jax.experimental import pallas as pl
from jax.experimental.pallas import tpu as pltpu
from jax.sharding import PartitionSpec as P

CAP_FACTOR = 2
F32, BF16 = jnp.float32, jnp.bfloat16
MESH = pl.DeviceIdType.MESH


def _grid_dims(n):
    return n // 32, 4, 4, 2


def _send_order(n):
    nz, ny, nx, nc = _grid_dims(n)
    hops = lambda a, m: min(a % m, m - a % m)
    dist = lambda o: hops(o[0], nz) + hops(o[1], ny) + hops(o[2], nx)
    todo = [(z, y, x, c) for z in range(nz) for y in range(ny) for x in range(nx) for c in range(nc)][1:]
    seen, order = set(), []
    for z, y, x, c in sorted(todo, key=lambda o: (-dist(o), o)):
        for a, b, d in ((z, y, x), (y, x, z), (x, z, y)):
            for s in (1, -1):
                q = (s * a % nz, s * b % ny, s * d % nx, c)
                if q not in seen and any(q):
                    seen.add(q)
                    order.append(q)
    assert sorted(order) == sorted(todo)
    return order


def _shift(me, n, offset, sign):
    nz, ny, nx, nc = _grid_dims(n)
    dz, dy, dx, dc = offset
    if sign < 0:
        dz, dy, dx = (nz - dz) % nz, (ny - dy) % ny, (nx - dx) % nx
    z, y, x, c = me // (ny * nx * nc), (me // (nx * nc)) % ny, (me // nc) % nx, me % nc
    return (((z + dz) % nz * ny + (y + dy) % ny) * nx + (x + dx) % nx) * nc + (c + dc) % nc


def _route_pack(src_cap, logits_ref, x_ref, send_ref, meta_ref, cnt_ref, slot_row):
    step = pl.program_id(0)

    @pl.when(step == 0)
    def _():
        lg = logits_ref[...]
        tok, experts = lg.shape
        lane = lax.broadcasted_iota(jnp.int32, lg.shape, 1)
        m1 = jnp.max(lg, axis=1, keepdims=True)
        i1 = jnp.min(jnp.where(lg == m1, lane, experts), axis=1, keepdims=True)
        rest = jnp.where(lane == i1, -jnp.inf, lg)
        m2 = jnp.max(rest, axis=1, keepdims=True)
        i2 = jnp.min(jnp.where(rest == m2, lane, experts), axis=1, keepdims=True)
        hot1, hot2 = lane == i1, lane == i2
        chosen = jnp.where(hot1 | hot2, 1.0, 0.0)
        total = jnp.sum(jnp.exp(lg - m1), axis=1, keepdims=True)
        g1 = 1.0 / total
        g2 = jnp.exp(m2 - m1) / total
        later = lax.broadcasted_iota(jnp.int32, (tok, tok), 0)
        early = lax.broadcasted_iota(jnp.int32, (tok, tok), 1)
        tri = jnp.where(early < later, 1.0, 0.0).astype(BF16)
        before = jnp.dot(tri, chosen.astype(BF16), preferred_element_type=F32)
        p1 = jnp.sum(jnp.where(hot1, before, 0.0), axis=1, keepdims=True)
        p2 = jnp.sum(jnp.where(hot2, before, 0.0), axis=1, keepdims=True)
        cnt_ref[...] = jnp.sum(chosen, axis=0, keepdims=True)
        e1, e2 = i1.astype(F32), i2.astype(F32)
        meta = jnp.where(lane == 0, g1, jnp.where(lane == 1, g2, jnp.where(lane == 2, e1, jnp.where(
            lane == 3, e2, jnp.where(lane == 4, p1, jnp.where(lane == 5, p2, jnp.where(
                lane == 6, e1 * src_cap + p1, jnp.where(lane == 7, e2 * src_cap + p2, 0.0))))))))
        meta_ref[...] = meta
        slot_row[...] = meta.T[0:8, :].astype(jnp.int32)

    rows = send_ref.shape[0]
    slot = lax.broadcasted_iota(jnp.int32, (rows, x_ref.shape[0]), 0) + step * rows
    pick = (slot == slot_row[6:7, :]) | (slot == slot_row[7:8, :])
    hot = jnp.where(pick, 1.0, 0.0).astype(BF16)
    send_ref[...] = jnp.dot(hot, x_ref[...], preferred_element_type=F32).astype(BF16)


def _exchange(n, group, send_ref, cnt_ref, w1_ref, w2_ref, ret_ref, all_ref, got_ref, rows_ref, z_ref,
              out_sem, got_sem, back_sem, ret_sem, cnt_out, cnt_got, own_sem, load_sem):
    me = lax.axis_index("ep")
    order = _send_order(n)
    cap = send_ref.shape[1]

    bar = pltpu.get_barrier_semaphore()

    def greet(k, carry):
        pl.semaphore_signal(bar, inc=1, device_id={"ep": (me + k) % n}, device_id_type=MESH)
        return carry

    lax.fori_loop(1, n, greet, 0)
    pl.semaphore_wait(bar, n - 1)

    def tell(k, carry):
        pltpu.make_async_remote_copy(cnt_ref, all_ref.at[me], cnt_out, cnt_got, device_id={"ep": (me + k) % n},
                                     device_id_type=MESH).start()
        return carry

    lax.fori_loop(1, n, tell, 0)
    for i, off in enumerate(order):
        peer = _shift(me, n, off, 1)
        pltpu.make_async_remote_copy(send_ref.at[peer], got_ref.at[i], out_sem, got_sem.at[i // group],
                                     device_id={"ep": peer}, device_id_type=MESH).start()
    own = pltpu.make_async_copy(send_ref.at[me], got_ref.at[n - 1], own_sem)
    own.start()
    own_cnt = pltpu.make_async_copy(cnt_ref, all_ref.at[me], own_sem)
    w1, w2 = w1_ref, w2_ref
    own.wait()
    own_cnt.start()
    own_cnt.wait()

    for g in range(n // group):
        lo = g * group
        cnt = min(group, n - 1 - lo)
        block = got_ref.at[pl.ds(lo, cnt)]
        pltpu.make_async_copy(block, block, got_sem.at[g]).wait()
        load = pltpu.make_async_copy(got_ref.at[pl.ds(lo, group)], rows_ref, load_sem)
        load.start()
        load.wait()
        x = rows_ref[...].reshape(group * cap, rows_ref.shape[2])
        h = jax.nn.gelu(jnp.dot(x, w1[...], preferred_element_type=F32), approximate=True).astype(BF16)
        z = jnp.dot(h, w2[...], preferred_element_type=F32).astype(BF16)
        z_ref[pl.ds(lo, group)] = z.reshape(group, cap, z.shape[1])
        for i in range(lo, lo + cnt):
            peer = _shift(me, n, order[i], -1)
            pltpu.make_async_remote_copy(z_ref.at[i], ret_ref.at[me], back_sem, ret_sem, device_id={"ep": peer},
                                         device_id_type=MESH).start()
    own_z = pltpu.make_async_copy(z_ref.at[n - 1], ret_ref.at[me], own_sem)
    own_z.start()
    own_z.wait()

    rest = pl.ds(0, n - 1)
    pltpu.make_async_copy(send_ref.at[rest], send_ref.at[rest], out_sem).wait()
    pltpu.make_async_copy(z_ref.at[rest], z_ref.at[rest], back_sem).wait()
    pltpu.make_async_copy(all_ref.at[rest], all_ref.at[rest], cnt_out).wait()
    pltpu.make_async_copy(all_ref.at[rest], all_ref.at[rest], cnt_got).wait()
    pltpu.make_async_copy(ret_ref.at[rest], ret_ref.at[rest], ret_sem).wait()


def _combine(capacity, src_cap, base_ref, ret_ref, x_ref, meta_ref, out_ref, pick1, pick2):
    @pl.when(pl.program_id(0) == 0)
    def _():
        meta = meta_ref[...]
        base = base_ref[...]
        lane = lax.broadcasted_iota(jnp.int32, meta.shape, 1).astype(F32)
        slots = lax.broadcasted_iota(jnp.int32, pick1.shape, 1).astype(F32)
        for c, pick in ((0, pick1), (1, pick2)):
            e, pos, slot = meta[:, 2 + c:3 + c], meta[:, 4 + c:5 + c], meta[:, 6 + c:7 + c]
            ahead = jnp.sum(jnp.where(lane == e, base, 0.0), axis=1, keepdims=True)
            slot = jnp.where(pos + ahead < capacity, slot, -1.0)
            pick[...] = jnp.where(slots == slot, 1.0, 0.0).astype(BF16)

    z = ret_ref[...]
    r1 = jnp.dot(pick1[...], z, preferred_element_type=F32)
    r2 = jnp.dot(pick2[...], z, preferred_element_type=F32)
    y = meta_ref[:, 0:1] * r1 + meta_ref[:, 1:2] * r2
    out_ref[...] = (x_ref[...].astype(F32) + y).astype(BF16)


def solution(mesh):
    n = mesh.shape["ep"]
    row_spec = P(("dp", "ep"), None)
    expert_spec = P("ep", None, None)

    def local_step(x_rows, logits, w_in, w_out):
        tok, d_model = x_rows.shape
        experts = logits.shape[1]
        ff = w_in.shape[2]
        capacity = CAP_FACTOR * tok * n // experts
        src_cap = 4 * tok // experts
        slots = experts * src_cap
        blk = 256
        whole = lambda *s: pl.BlockSpec(s, lambda i: (0,) * len(s))
        send, meta, cnt = pl.pallas_call(
            functools.partial(_route_pack, src_cap),
            grid=(slots // blk,),
            in_specs=[whole(tok, experts), whole(tok, d_model)],
            out_specs=[pl.BlockSpec((blk, d_model), lambda i: (i, 0)), whole(tok, experts), whole(1, experts)],
            out_shape=[jax.ShapeDtypeStruct((slots, d_model), BF16), jax.ShapeDtypeStruct((tok, experts), F32),
                       jax.ShapeDtypeStruct((1, experts), F32)],
            scratch_shapes=[pltpu.VMEM((8, tok), jnp.int32)],
            name="route_pack",
        )(logits, x_rows)

        group = 16
        any_ = pl.BlockSpec(memory_space=pl.ANY)
        vmem = pl.BlockSpec(memory_space=pltpu.VMEM)
        dma = pltpu.SemaphoreType.DMA
        ret, all_cnt, _ = pl.pallas_call(
            functools.partial(_exchange, n, group),
            in_specs=[any_, any_, vmem, vmem],
            out_specs=[any_, any_, any_],
            out_shape=[jax.ShapeDtypeStruct((n, src_cap, d_model), BF16), jax.ShapeDtypeStruct((n, 1, experts), F32),
                       jax.ShapeDtypeStruct((n, src_cap, d_model), BF16)],
            scratch_shapes=[pltpu.VMEM((group, src_cap, d_model), BF16), pltpu.VMEM((n, src_cap, d_model), BF16),
                            dma, dma((n // group,)), dma, dma, dma, dma, dma, dma],
            compiler_params=pltpu.CompilerParams(collective_id=0, has_side_effects=True, vmem_limit_bytes=60 * 2**20),
            name="exchange",
        )(send.reshape(n, src_cap, d_model), cnt, w_in[0], w_out[0])

        me = lax.axis_index("ep")
        ahead = (jnp.arange(n) < me).astype(F32)[:, None]
        base = jnp.sum(all_cnt[:, 0, :] * ahead, axis=0, keepdims=True)
        cols = 256
        return pl.pallas_call(
            functools.partial(_combine, capacity, src_cap),
            grid=(d_model // cols,),
            in_specs=[whole(1, experts), pl.BlockSpec((slots, cols), lambda i: (0, i)),
                      pl.BlockSpec((tok, cols), lambda i: (0, i)), whole(tok, experts)],
            out_specs=pl.BlockSpec((tok, cols), lambda i: (0, i)),
            out_shape=jax.ShapeDtypeStruct((tok, d_model), BF16),
            scratch_shapes=[pltpu.VMEM((tok, slots), BF16), pltpu.VMEM((tok, slots), BF16)],
            name="combine",
        )(base, ret.reshape(slots, d_model), x_rows, meta)

    return jax.shard_map(local_step, mesh=mesh, in_specs=(row_spec, row_spec, expert_spec, expert_spec),
                         out_specs=row_spec, check_vma=False)
```

```python
import functools
import jax
import jax.numpy as jnp
from jax import lax
from jax.experimental import pallas as pl
from jax.experimental.pallas import tpu as pltpu
from jax.sharding import PartitionSpec as P

CAP_FACTOR = 2
F32, BF16 = jnp.float32, jnp.bfloat16
MESH = pl.DeviceIdType.MESH
BF16_MAX = float(jnp.finfo(jnp.bfloat16).max)


def _grid_dims(n):
    return n // 32, 4, 4, 2


def _send_order(n):
    nz, ny, nx, nc = _grid_dims(n)
    hops = lambda a, m: min(a % m, m - a % m)
    dist = lambda o: hops(o[0], nz) + hops(o[1], ny) + hops(o[2], nx)
    todo = [(z, y, x, c) for z in range(nz) for y in range(ny) for x in range(nx) for c in range(nc)][1:]
    seen, order = set(), []
    for z, y, x, c in sorted(todo, key=lambda o: (-dist(o), o)):
        for a, b, d in ((z, y, x), (y, x, z), (x, z, y)):
            for s in (1, -1):
                q = (s * a % nz, s * b % ny, s * d % nx, c)
                if q not in seen and any(q):
                    seen.add(q)
                    order.append(q)
    assert sorted(order) == sorted(todo)
    return order


def _shift(me, n, offset, sign):
    nz, ny, nx, nc = _grid_dims(n)
    dz, dy, dx, dc = offset
    if sign < 0:
        dz, dy, dx = (nz - dz) % nz, (ny - dy) % ny, (nx - dx) % nx
    z, y, x, c = me // (ny * nx * nc), (me // (nx * nc)) % ny, (me // nc) % nx, me % nc
    return (((z + dz) % nz * ny + (y + dy) % ny) * nx + (x + dx) % nx) * nc + (c + dc) % nc


def _route_pack(src_cap, logits_ref, x_ref, send_ref, meta_ref, cnt_ref, slot_row):
    step = pl.program_id(0)

    @pl.when(step == 0)
    def _():
        lg = logits_ref[...]
        tok, experts = lg.shape
        lane = lax.broadcasted_iota(jnp.int32, lg.shape, 1)
        m1 = jnp.max(lg, axis=1, keepdims=True)
        i1 = jnp.min(jnp.where(lg == m1, lane, experts), axis=1, keepdims=True)
        rest = jnp.where(lane == i1, -jnp.inf, lg)
        m2 = jnp.max(rest, axis=1, keepdims=True)
        i2 = jnp.min(jnp.where(rest == m2, lane, experts), axis=1, keepdims=True)
        hot1, hot2 = lane == i1, lane == i2
        chosen = jnp.where(hot1 | hot2, 1.0, 0.0)
        total = jnp.sum(jnp.exp(lg - m1), axis=1, keepdims=True)
        g1 = 1.0 / total
        g2 = jnp.exp(m2 - m1) / total
        later = lax.broadcasted_iota(jnp.int32, (tok, tok), 0)
        early = lax.broadcasted_iota(jnp.int32, (tok, tok), 1)
        tri = jnp.where(early < later, 1.0, 0.0).astype(BF16)
        before = jnp.dot(tri, chosen.astype(BF16), preferred_element_type=F32)
        p1 = jnp.sum(jnp.where(hot1, before, 0.0), axis=1, keepdims=True)
        p2 = jnp.sum(jnp.where(hot2, before, 0.0), axis=1, keepdims=True)
        cnt_ref[...] = jnp.sum(chosen, axis=0, keepdims=True)
        e1, e2 = i1.astype(F32), i2.astype(F32)
        meta = jnp.where(lane == 0, g1, jnp.where(lane == 1, g2, jnp.where(lane == 2, e1, jnp.where(
            lane == 3, e2, jnp.where(lane == 4, p1, jnp.where(lane == 5, p2, jnp.where(
                lane == 6, e1 * src_cap + p1, jnp.where(lane == 7, e2 * src_cap + p2, 0.0))))))))
        meta_ref[...] = meta
        slot_row[...] = meta.T[0:8, :].astype(jnp.int32)

    rows = send_ref.shape[0]
    slot = lax.broadcasted_iota(jnp.int32, (rows, x_ref.shape[0]), 0) + step * rows
    pick = (slot == slot_row[6:7, :]) | (slot == slot_row[7:8, :])
    hot = jnp.where(pick, 1.0, 0.0).astype(BF16)
    send_ref[...] = jnp.dot(hot, x_ref[...], preferred_element_type=F32).astype(BF16)


def _exchange(n, group, send_ref, cnt_ref, w1_ref, w2_ref, ret_ref, all_ref, got_ref, zh_ref, rows, zv,
              out_sem, got_sem, back_sem, ret_sem, cnt_out, cnt_got, own_sem, load_sem, store_sem):
    me = lax.axis_index("ep")
    order = _send_order(n)
    cap, d_model = send_ref.shape[1:]
    chunks = n // group

    bar = pltpu.get_barrier_semaphore()

    def greet(k, carry):
        pl.semaphore_signal(bar, inc=1, device_id={"ep": (me + k) % n}, device_id_type=MESH)
        return carry

    lax.fori_loop(1, n, greet, 0)
    pl.semaphore_wait(bar, n - 1)

    def span(j):
        return range(j * group, min((j + 1) * group, n - 1))

    for j in range(chunks):
        for i in span(j):
            peer = _shift(me, n, order[i], 1)
            pltpu.make_async_remote_copy(send_ref.at[peer], got_ref.at[i], out_sem, got_sem.at[j],
                                         device_id={"ep": peer}, device_id_type=MESH).start()

    def tell(k, carry):
        pltpu.make_async_remote_copy(cnt_ref, all_ref.at[me], cnt_out, cnt_got, device_id={"ep": (me + k) % n},
                                     device_id_type=MESH).start()
        return carry

    lax.fori_loop(1, n, tell, 0)
    own = pltpu.make_async_copy(send_ref.at[me], got_ref.at[n - 1], own_sem)
    own.start()
    own.wait()
    own_cnt = pltpu.make_async_copy(cnt_ref, all_ref.at[me], own_sem)
    own_cnt.start()
    own_cnt.wait()

    def z_store(j):
        return pltpu.make_async_copy(zv.at[j % 2], zh_ref.at[pl.ds(j * group, group)], store_sem.at[j % 2])

    def back(j):
        z_store(j).wait()
        for i in span(j):
            pltpu.make_async_remote_copy(zh_ref.at[i], ret_ref.at[me], back_sem, ret_sem,
                                         device_id={"ep": _shift(me, n, order[i], -1)}, device_id_type=MESH).start()

    for j in range(chunks):
        block = got_ref.at[pl.ds(j * group, len(span(j)))]
        pltpu.make_async_copy(block, block, got_sem.at[j]).wait()
        load = pltpu.make_async_copy(got_ref.at[pl.ds(j * group, group)], rows, load_sem)
        load.start()
        if j > 0:
            back(j - 1)
        load.wait()
        xs = rows[...].reshape(group * cap, d_model)
        h = jax.nn.gelu(jnp.dot(xs, w1_ref[...], preferred_element_type=F32), approximate=True).astype(BF16)
        z = jnp.dot(h, w2_ref[...], preferred_element_type=F32)
        z = jnp.clip(z, -BF16_MAX, BF16_MAX)
        zv[j % 2] = z.astype(BF16).reshape(group, cap, d_model)
        z_store(j).start()
    back(chunks - 1)
    own_z = pltpu.make_async_copy(zv.at[(chunks - 1) % 2, group - 1], ret_ref.at[me], own_sem)
    own_z.start()
    own_z.wait()

    rest = pl.ds(0, n - 1)
    pltpu.make_async_copy(send_ref.at[rest], send_ref.at[rest], out_sem).wait()
    pltpu.make_async_copy(zh_ref.at[rest], zh_ref.at[rest], back_sem).wait()
    pltpu.make_async_copy(all_ref.at[rest], all_ref.at[rest], cnt_out).wait()
    pltpu.make_async_copy(all_ref.at[rest], all_ref.at[rest], cnt_got).wait()
    pltpu.make_async_copy(ret_ref.at[rest], ret_ref.at[rest], ret_sem).wait()


def _combine(capacity, base_ref, ret_ref, x_ref, meta_ref, out_ref, pick):
    tok = x_ref.shape[0]

    @pl.when(pl.program_id(0) == 0)
    def _():
        meta = meta_ref[...]
        base = base_ref[...]
        lane = lax.broadcasted_iota(jnp.int32, meta.shape, 1).astype(F32)
        slots = lax.broadcasted_iota(jnp.int32, (tok, pick.shape[1]), 1).astype(F32)
        for c in range(2):
            e, pos, slot = meta[:, 2 + c:3 + c], meta[:, 4 + c:5 + c], meta[:, 6 + c:7 + c]
            ahead = jnp.sum(jnp.where(lane == e, base, 0.0), axis=1, keepdims=True)
            slot = jnp.where(pos + ahead < capacity, slot, -1.0)
            pick[c * tok:(c + 1) * tok, :] = jnp.where(slots == slot, 1.0, 0.0).astype(BF16)

    z = ret_ref[...]
    z = jnp.where(z == z, z, jnp.zeros_like(z))
    r = jnp.dot(pick[...], z, preferred_element_type=F32)
    y = meta_ref[:, 0:1] * r[0:tok] + meta_ref[:, 1:2] * r[tok:2 * tok]
    out_ref[...] = (x_ref[...].astype(F32) + y).astype(BF16)


def solution(mesh):
    n = mesh.shape["ep"]
    row_spec = P(("dp", "ep"), None)
    expert_spec = P("ep", None, None)

    def local_step(x_rows, logits, w_in, w_out):
        tok, d_model = x_rows.shape
        experts = logits.shape[1]
        ff = w_in.shape[2]
        capacity = CAP_FACTOR * tok * n // experts
        src_cap = 4 * tok // experts
        slots = experts * src_cap
        blk = 256
        whole = lambda *s: pl.BlockSpec(s, lambda i: (0,) * len(s))
        send, meta, cnt = pl.pallas_call(
            functools.partial(_route_pack, src_cap),
            grid=(slots // blk,),
            in_specs=[whole(tok, experts), whole(tok, d_model)],
            out_specs=[pl.BlockSpec((blk, d_model), lambda i: (i, 0)), whole(tok, experts), whole(1, experts)],
            out_shape=[jax.ShapeDtypeStruct((slots, d_model), BF16), jax.ShapeDtypeStruct((tok, experts), F32),
                       jax.ShapeDtypeStruct((1, experts), F32)],
            scratch_shapes=[pltpu.VMEM((8, tok), jnp.int32)],
            name="route_pack",
        )(logits, x_rows)

        group = 16
        any_ = pl.BlockSpec(memory_space=pl.ANY)
        vmem = pl.BlockSpec(memory_space=pltpu.VMEM)
        dma = pltpu.SemaphoreType.DMA
        ret, all_cnt, _, _ = pl.pallas_call(
            functools.partial(_exchange, n, group),
            in_specs=[any_, any_, vmem, vmem],
            out_specs=[any_, any_, any_, any_],
            out_shape=[jax.ShapeDtypeStruct((n, src_cap, d_model), BF16), jax.ShapeDtypeStruct((n, 1, experts), F32),
                       jax.ShapeDtypeStruct((n, src_cap, d_model), BF16),
                       jax.ShapeDtypeStruct((n, src_cap, d_model), BF16)],
            scratch_shapes=[pltpu.VMEM((group, src_cap, d_model), BF16), pltpu.VMEM((2, group, src_cap, d_model), BF16),
                            dma, dma((n // group,)), dma, dma, dma, dma, dma, dma, dma((2,))],
            compiler_params=pltpu.CompilerParams(collective_id=0, has_side_effects=True, vmem_limit_bytes=60 * 2**20),
            name="exchange",
        )(send.reshape(n, src_cap, d_model), cnt, w_in[0], w_out[0])

        me = lax.axis_index("ep")
        ahead = (jnp.arange(n) < me).astype(F32)[:, None]
        base = jnp.sum(all_cnt[:, 0, :] * ahead, axis=0, keepdims=True)
        cols = 256
        return pl.pallas_call(
            functools.partial(_combine, capacity),
            grid=(d_model // cols,),
            in_specs=[whole(1, experts), pl.BlockSpec((slots, cols), lambda i: (0, i)),
                      pl.BlockSpec((tok, cols), lambda i: (0, i)), whole(tok, experts)],
            out_specs=pl.BlockSpec((tok, cols), lambda i: (0, i)),
            out_shape=jax.ShapeDtypeStruct((tok, d_model), BF16),
            scratch_shapes=[pltpu.VMEM((2 * tok, slots), BF16)],
            name="combine",
        )(base, ret.reshape(slots, d_model), x_rows, meta)

    return jax.shard_map(local_step, mesh=mesh, in_specs=(row_spec, row_spec, expert_spec, expert_spec),
                         out_specs=row_spec, check_vma=False)
```

```python
import functools
import jax
import jax.numpy as jnp
import numpy as np
from jax import lax
from jax.experimental import pallas as pl
from jax.experimental.pallas import tpu as pltpu
from jax.sharding import PartitionSpec as P

CAP_FACTOR = 2
F32, BF16, I32 = jnp.float32, jnp.bfloat16, jnp.int32
MESH = pl.DeviceIdType.MESH
BF16_MAX = float(jnp.finfo(jnp.bfloat16).max)
SIDE, CORES = 4, 2


def _send_order(chips):
    nz = chips // SIDE**2
    hops = lambda a, m: min(a % m, m - a % m)
    dist = lambda o: hops(o[0], nz) + hops(o[1], SIDE) + hops(o[2], SIDE)
    todo = [(z, y, x) for z in range(nz) for y in range(SIDE) for x in range(SIDE)][1:]
    seen, order = set(), []
    for z, y, x in sorted(todo, key=lambda o: (-dist(o), o)):
        for a, b, d in ((z, y, x), (y, x, z), (x, z, y)):
            for s in (1, -1):
                q = (s * a % nz, s * b % SIDE, s * d % SIDE)
                if q not in seen and any(q):
                    seen.add(q)
                    order.append(q)
    assert sorted(order) == sorted(todo)
    return order + [(0, 0, 0)]


def _chip_at(chip, chips, dz, dy, dx):
    nz = chips // SIDE**2
    z, y, x = chip // SIDE**2, (chip // SIDE) % SIDE, chip % SIDE
    return ((z + dz) % nz * SIDE + (y + dy) % SIDE) * SIDE + (x + dx) % SIDE


def _route_pack(n, cap, logits_ref, x_ref, off_ref, send_ref, hot_ref, meta_ref, cnt_ref):
    step = pl.program_id(0)
    tok, experts = logits_ref.shape

    @pl.when(step == 0)
    def _():
        lg = logits_ref[...]
        lane = lax.broadcasted_iota(I32, lg.shape, 1)
        m1 = jnp.max(lg, axis=1, keepdims=True)
        i1 = jnp.min(jnp.where(lg == m1, lane, experts), axis=1, keepdims=True)
        rest = jnp.where(lane == i1, -jnp.inf, lg)
        m2 = jnp.max(rest, axis=1, keepdims=True)
        i2 = jnp.min(jnp.where(rest == m2, lane, experts), axis=1, keepdims=True)
        hot1, hot2 = lane == i1, lane == i2
        chosen = jnp.where(hot1 | hot2, 1.0, 0.0)
        total = jnp.sum(jnp.exp(lg - m1), axis=1, keepdims=True)
        later = lax.broadcasted_iota(I32, (tok, tok), 0)
        early = lax.broadcasted_iota(I32, (tok, tok), 1)
        tri = jnp.where(early < later, 1.0, 0.0).astype(BF16)
        before = jnp.dot(tri, chosen.astype(BF16), preferred_element_type=F32)
        p1 = jnp.sum(jnp.where(hot1, before, 0.0), axis=1, keepdims=True)
        p2 = jnp.sum(jnp.where(hot2, before, 0.0), axis=1, keepdims=True)
        e1, e2 = i1.astype(F32), i2.astype(F32)
        cnt_ref[...] = jnp.sum(chosen, axis=0, keepdims=True)
        table = jnp.zeros_like(lg)
        for k, col in enumerate((1.0 / total, jnp.exp(m2 - m1) / total, e1, e2, p1, p2, e1 * cap + p1, e2 * cap + p2)):
            table = jnp.where(lane == k, col, table)
        meta_ref[...] = table

    off = off_ref[pl.ds(step, 1)].reshape(1, send_ref.shape[0])
    chip = lax.axis_index("ep") // CORES
    z, y, x = chip // SIDE**2, (chip // SIDE) % SIDE, chip % SIDE
    chips = n // CORES
    nz = chips // SIDE**2
    dz, dy, dx = off // SIDE**2, (off // SIDE) % SIDE, off % SIDE
    other = ((z + dz) % nz * SIDE + (y + dy) % SIDE) * SIDE + (x + dx) % SIDE
    place = lax.broadcasted_iota(I32, off.shape, 1) % (CORES * cap)
    slot = (other * (CORES * cap) + place).astype(F32)
    first = jnp.where(meta_ref[:, 6:7] == slot, 1.0, 0.0)
    second = jnp.where(meta_ref[:, 7:8] == slot, 1.0, 0.0)
    hot_ref[0:tok, :] = first.astype(BF16)
    hot_ref[tok:2 * tok, :] = second.astype(BF16)
    send_ref[...] = lax.dot_general((first + second).astype(BF16), x_ref[...], (((0,), (0,)), ((), ())),
                                    preferred_element_type=F32).astype(BF16)


def _exchange(n, group, send_ref, cnt_ref, hot_hbm, w1_ref, w2_ref, picked_ref, all_ref, got_ref, side_ref, zp_ref, ret_ref,
              rows, zv, hot, out_sem, got_sem, fw_out, fw_got, z_out, z_got, back_sem, ret_sem, cnt_out, cnt_got,
              own_sem, load_sem, store_sem):
    me = lax.axis_index("ep")
    chips = n // CORES
    chip, core = me // CORES, me % CORES
    sibling = chip * CORES + 1 - core
    order = _send_order(chips)
    cap, d_model = send_ref.shape[1:]
    half = group // CORES
    chunks = chips // half

    bar = pltpu.get_barrier_semaphore()

    def greet(k, carry):
        pl.semaphore_signal(bar, inc=1, device_id={"ep": (me + k) % n}, device_id_type=MESH)
        return carry

    lax.fori_loop(1, n, greet, 0)
    pl.semaphore_wait(bar, n - 1)

    def span(j):
        return range(j * half, min((j + 1) * half, chips - 1))

    def remote(src, dst, out, got, to):
        return pltpu.make_async_remote_copy(src, dst, out, got, device_id={"ep": to}, device_id_type=MESH)

    def pair(i):
        return pl.ds(i * CORES, CORES)

    for j in range(chunks):
        for i in span(j):
            to = _chip_at(chip, chips, *order[i]) * CORES + core
            remote(send_ref.at[pair(i)], got_ref.at[i], out_sem, got_sem.at[j], to).start()

    def tell(k, carry):
        remote(cnt_ref, all_ref.at[me], cnt_out, cnt_got, (me + k) % n).start()
        return carry

    lax.fori_loop(1, n, tell, 0)
    own = pltpu.make_async_copy(send_ref.at[pair(chips - 1)], got_ref.at[chips - 1], own_sem)
    own.start()
    own.wait()
    own_cnt = pltpu.make_async_copy(cnt_ref, all_ref.at[me], own_sem)
    own_cnt.start()
    own_cnt.wait()

    def some(j):
        return pl.ds(j * half, half)

    def hand(j):
        return remote(got_ref.at[some(j), 1 - core], side_ref.at[some(j)], fw_out, fw_got.at[j], sibling)

    def z_store(j):
        return pltpu.make_async_copy(zv.at[j % 2, pl.ds(0, half)], zp_ref.at[some(j), core], store_sem.at[j % 2])

    def z_hand(j):
        return remote(zv.at[j % 2, pl.ds(half, half)], zp_ref.at[some(j), core], z_out.at[j % 2], z_got.at[j], sibling)

    def back(j):
        z_store(j).wait()
        z_hand(j).wait_send()
        z_hand(j).wait_recv()
        for i in span(j):
            dz, dy, dx = order[i]
            to = _chip_at(chip, chips, chips // SIDE**2 - dz, SIDE - dy, SIDE - dx) * CORES + core
            remote(zp_ref.at[i], ret_ref.at[pair(i)], back_sem, ret_sem.at[j], to).start()

    for j in range(chunks + 1):
        if j < chunks:
            block = got_ref.at[pl.ds(j * half, len(span(j)))]
            pltpu.make_async_copy(block, block, got_sem.at[j]).wait()
            hand(j).start()
        if j == 0:
            continue
        p = j - 1
        direct = pltpu.make_async_copy(got_ref.at[some(p), core], rows.at[pl.ds(0, half)], load_sem.at[0])
        direct.start()
        hand(p).wait_recv()
        handed = pltpu.make_async_copy(side_ref.at[some(p)], rows.at[pl.ds(half, half)], load_sem.at[1])
        handed.start()
        if p > 0:
            back(p - 1)
        direct.wait()
        handed.wait()
        xs = rows[...].reshape(group * cap, d_model)
        h = jax.nn.gelu(jnp.dot(xs, w1_ref[...], preferred_element_type=F32), approximate=True).astype(BF16)
        z = jnp.dot(h, w2_ref[...], preferred_element_type=F32)
        z = jnp.clip(z, -BF16_MAX, BF16_MAX)
        zv[p % 2] = z.astype(BF16).reshape(group, cap, d_model)
        z_store(p).start()
        z_hand(p).start()
    back(chunks - 1)
    own_z = pltpu.make_async_copy(zp_ref.at[chips - 1], ret_ref.at[pair(chips - 1)], own_sem)
    own_z.start()
    own_z.wait()

    for j in range(chunks):
        lo = j * group
        block = ret_ref.at[pl.ds(lo, len(span(j)) * CORES)]
        get_hot = pltpu.make_async_copy(hot_hbm.at[j], hot, load_sem.at[1])
        get_hot.start()
        pltpu.make_async_copy(block, block, ret_sem.at[j]).wait()
        load = pltpu.make_async_copy(ret_ref.at[pl.ds(lo, group)], rows, load_sem.at[0])
        load.start()
        get_hot.wait()
        load.wait()
        part = jnp.dot(hot[...], rows[...].reshape(group * cap, d_model), preferred_element_type=F32).astype(BF16)
        picked_ref[...] = part if j == 0 else picked_ref[...] + part

    most = pl.ds(0, (chips - 1) * CORES)
    rest = pl.ds(0, n - 1)
    pltpu.make_async_copy(send_ref.at[most], send_ref.at[most], out_sem).wait()
    pltpu.make_async_copy(side_ref, side_ref, fw_out).wait()
    pltpu.make_async_copy(ret_ref.at[most], ret_ref.at[most], back_sem).wait()
    pltpu.make_async_copy(all_ref.at[rest], all_ref.at[rest], cnt_out).wait()
    pltpu.make_async_copy(all_ref.at[rest], all_ref.at[rest], cnt_got).wait()


def _finish(capacity, all_ref, x_ref, meta_ref, one_ref, two_ref, out_ref):
    me = lax.axis_index("ep")
    early = lax.broadcasted_iota(I32, all_ref.shape, 0) < me
    base = jnp.sum(jnp.where(early, all_ref[...], 0.0), axis=0)
    meta = meta_ref[...]
    lane = lax.broadcasted_iota(I32, meta.shape, 1).astype(F32)
    y = 0.0
    for k, z_ref in enumerate((one_ref, two_ref)):
        e, pos = meta[:, 2 + k:3 + k], meta[:, 4 + k:5 + k]
        before = pos + jnp.sum(jnp.where(lane == e, base, 0.0), axis=1, keepdims=True)
        y += jnp.where(before < capacity, meta[:, k:k + 1], 0.0) * z_ref[...].astype(F32)
    out_ref[...] = (x_ref[...].astype(F32) + y).astype(BF16)


def solution(mesh):
    n = mesh.shape["ep"]
    row_spec = P(("dp", "ep"), None)
    expert_spec = P("ep", None, None)

    def local_step(x_rows, logits, w_in, w_out):
        tok, d_model = x_rows.shape
        experts = logits.shape[1]
        capacity = CAP_FACTOR * tok * n // experts
        cap = 4 * tok // experts
        group = 16
        chips, chunks, width = n // CORES, n // group, group * cap
        code = np.array([(z * SIDE + y) * SIDE + x for z, y, x in _send_order(chips)], np.int32)
        offsets = jnp.asarray(np.repeat(code, CORES * cap).reshape(chunks, 1, width))
        whole = lambda *s: pl.BlockSpec(s, lambda i: (0,) * len(s))
        send, hot, meta, cnt = pl.pallas_call(
            functools.partial(_route_pack, n, cap),
            grid=(chunks,),
            in_specs=[whole(tok, experts), whole(tok, d_model), whole(chunks, 1, width)],
            out_specs=[pl.BlockSpec((width, d_model), lambda i: (i, 0)), pl.BlockSpec((2 * tok, width), lambda i: (i, 0)),
                       whole(tok, experts), whole(1, experts)],
            out_shape=[jax.ShapeDtypeStruct((chunks * width, d_model), BF16),
                       jax.ShapeDtypeStruct((chunks * 2 * tok, width), BF16),
                       jax.ShapeDtypeStruct((tok, experts), F32), jax.ShapeDtypeStruct((1, experts), F32)],
            name="route_pack",
        )(logits, x_rows, offsets)

        any_ = pl.BlockSpec(memory_space=pl.ANY)
        vmem = pl.BlockSpec(memory_space=pltpu.VMEM)
        dma = pltpu.SemaphoreType.DMA
        pairs = jax.ShapeDtypeStruct((chips, CORES, cap, d_model), BF16)
        picked, all_cnt = pl.pallas_call(
            functools.partial(_exchange, n, group),
            in_specs=[any_, any_, any_, vmem, vmem],
            out_specs=[vmem, any_, any_, any_, any_, any_],
            out_shape=[jax.ShapeDtypeStruct((2 * tok, d_model), BF16), jax.ShapeDtypeStruct((n, 1, experts), F32),
                       pairs, jax.ShapeDtypeStruct((chips, cap, d_model), BF16), pairs,
                       jax.ShapeDtypeStruct((n, cap, d_model), BF16)],
            scratch_shapes=[pltpu.VMEM((group, cap, d_model), BF16), pltpu.VMEM((2, group, cap, d_model), BF16),
                            pltpu.VMEM((2 * tok, width), BF16),
                            dma, dma((chunks,)), dma, dma((chunks,)), dma((2,)), dma((chunks,)), dma, dma((chunks,)),
                            dma, dma, dma, dma((2,)), dma((2,))],
            compiler_params=pltpu.CompilerParams(collective_id=0, has_side_effects=True, vmem_limit_bytes=60 * 2**20),
            name="exchange",
        )(send.reshape(n, cap, d_model), cnt, hot.reshape(chunks, 2 * tok, width), w_in[0], w_out[0])[:2]

        blk = tok // 4
        part = lambda s: pl.BlockSpec((blk, d_model), lambda i: (i + s, 0))
        return pl.pallas_call(
            functools.partial(_finish, capacity),
            grid=(tok // blk,),
            in_specs=[whole(n, 1, experts), part(0), pl.BlockSpec((blk, experts), lambda i: (i, 0)), part(0),
                      part(tok // blk)],
            out_specs=part(0),
            out_shape=jax.ShapeDtypeStruct((tok, d_model), BF16),
            name="finish",
        )(all_cnt, x_rows, meta, picked, picked)

    return jax.shard_map(local_step, mesh=mesh, in_specs=(row_spec, row_spec, expert_spec, expert_spec),
                         out_specs=row_spec, check_vma=False)
```

```python
import functools
import jax
import jax.numpy as jnp
import numpy as np
from jax import lax
from jax.experimental import pallas as pl
from jax.experimental.pallas import tpu as pltpu
from jax.sharding import PartitionSpec as P

CAP_FACTOR = 2
F32, BF16, I32 = jnp.float32, jnp.bfloat16, jnp.int32
MESH = pl.DeviceIdType.MESH
BF16_MAX = float(jnp.finfo(jnp.bfloat16).max)
SIDE, CORES = 4, 2


def _send_order(n):
    nz = n // (SIDE * SIDE * CORES)
    hops = lambda a, m: min(a % m, m - a % m)
    dist = lambda o: hops(o[0], nz) + hops(o[1], SIDE) + hops(o[2], SIDE)
    todo = [(z, y, x, c) for z in range(nz) for y in range(SIDE) for x in range(SIDE) for c in range(CORES)][1:]
    seen, order = set(), []
    for z, y, x, c in sorted(todo, key=lambda o: (-dist(o), o)):
        for a, b, d in ((z, y, x), (y, x, z), (x, z, y)):
            for s in (1, -1):
                q = (s * a % nz, s * b % SIDE, s * d % SIDE, c)
                if q not in seen and any(q):
                    seen.add(q)
                    order.append(q)
    assert sorted(order) == sorted(todo)
    return order + [(0, 0, 0, 0)]


def _device_at(me, n, dz, dy, dx, dc):
    nz = n // (SIDE * SIDE * CORES)
    z, y, x, c = me // (SIDE * SIDE * CORES), me // (SIDE * CORES) % SIDE, me // CORES % SIDE, me % CORES
    return (((z + dz) % nz * SIDE + (y + dy) % SIDE) * SIDE + (x + dx) % SIDE) * CORES + (c + dc) % CORES


def _route_pack(n, cap, logits_ref, x_ref, off_ref, send_ref, hot_ref, meta_ref, cnt_ref):
    step = pl.program_id(0)
    tok, experts = logits_ref.shape

    @pl.when(step == 0)
    def _():
        lg = logits_ref[...]
        lane = lax.broadcasted_iota(I32, lg.shape, 1)
        m1 = jnp.max(lg, axis=1, keepdims=True)
        i1 = jnp.min(jnp.where(lg == m1, lane, experts), axis=1, keepdims=True)
        rest = jnp.where(lane == i1, -jnp.inf, lg)
        m2 = jnp.max(rest, axis=1, keepdims=True)
        i2 = jnp.min(jnp.where(rest == m2, lane, experts), axis=1, keepdims=True)
        hot1, hot2 = lane == i1, lane == i2
        chosen = jnp.where(hot1 | hot2, 1.0, 0.0)
        total = jnp.sum(jnp.exp(lg - m1), axis=1, keepdims=True)
        later = lax.broadcasted_iota(I32, (tok, tok), 0)
        early = lax.broadcasted_iota(I32, (tok, tok), 1)
        tri = jnp.where(early < later, 1.0, 0.0).astype(BF16)
        before = jnp.dot(tri, chosen.astype(BF16), preferred_element_type=F32)
        p1 = jnp.sum(jnp.where(hot1, before, 0.0), axis=1, keepdims=True)
        p2 = jnp.sum(jnp.where(hot2, before, 0.0), axis=1, keepdims=True)
        e1, e2 = i1.astype(F32), i2.astype(F32)
        cnt_ref[...] = jnp.sum(chosen, axis=0, keepdims=True)
        table = jnp.zeros_like(lg)
        for k, col in enumerate((1.0 / total, jnp.exp(m2 - m1) / total, e1, e2, p1, p2, e1 * cap + p1, e2 * cap + p2)):
            table = jnp.where(lane == k, col, table)
        meta_ref[...] = table

    off = off_ref[pl.ds(step, 1)].reshape(1, send_ref.shape[0])
    me = lax.axis_index("ep")
    dz, dy, dx, dc = off // (SIDE * SIDE * CORES), off // (SIDE * CORES) % SIDE, off // CORES % SIDE, off % CORES
    other = _device_at(me, n, dz, dy, dx, dc)
    place = lax.broadcasted_iota(I32, off.shape, 1) % cap
    slot = (other * cap + place).astype(F32)
    first = jnp.where(meta_ref[:, 6:7] == slot, 1.0, 0.0)
    second = jnp.where(meta_ref[:, 7:8] == slot, 1.0, 0.0)
    hot_ref[0:tok, :] = first.astype(BF16)
    hot_ref[tok:2 * tok, :] = second.astype(BF16)
    send_ref[...] = lax.dot_general((first + second).astype(BF16), x_ref[...], (((0,), (0,)), ((), ())),
                                    preferred_element_type=F32).astype(BF16)


def _exchange(n, group, send_ref, cnt_ref, hot_hbm, w1_ref, w2_ref, picked_ref, all_ref, got_ref, zh_ref, ret_ref,
              rows, zv, hot, out_sem, got_sem, back_sem, ret_sem, cnt_out, cnt_got, own_sem, load_sem, store_sem):
    me = lax.axis_index("ep")
    order = _send_order(n)
    cap, d_model = send_ref.shape[1:]
    chunks = n // group

    bar = pltpu.get_barrier_semaphore()

    def greet(k, carry):
        pl.semaphore_signal(bar, inc=1, device_id={"ep": (me + k) % n}, device_id_type=MESH)
        return carry

    lax.fori_loop(1, n, greet, 0)
    pl.semaphore_wait(bar, n - 1)

    def span(j):
        return range(j * group, min((j + 1) * group, n - 1))

    def remote(src, dst, out, got, to):
        return pltpu.make_async_remote_copy(src, dst, out, got, device_id={"ep": to}, device_id_type=MESH)

    for j in range(chunks):
        for i in span(j):
            remote(send_ref.at[i], got_ref.at[i], out_sem, got_sem.at[j], _device_at(me, n, *order[i])).start()

    def tell(k, carry):
        remote(cnt_ref, all_ref.at[me], cnt_out, cnt_got, (me + k) % n).start()
        return carry

    lax.fori_loop(1, n, tell, 0)
    own = pltpu.make_async_copy(send_ref.at[n - 1], got_ref.at[n - 1], own_sem)
    own.start()
    own.wait()
    own_cnt = pltpu.make_async_copy(cnt_ref, all_ref.at[me], own_sem)
    own_cnt.start()
    own_cnt.wait()

    def some(j):
        return pl.ds(j * group, group)

    def z_store(j):
        return pltpu.make_async_copy(zv.at[j % 2], zh_ref.at[some(j)], store_sem.at[j % 2])

    def back(j):
        z_store(j).wait()
        for i in span(j):
            dz, dy, dx, dc = order[i]
            to = _device_at(me, n, n - dz, n - dy, n - dx, n - dc)
            remote(zh_ref.at[i], ret_ref.at[i], back_sem, ret_sem.at[j], to).start()

    for j in range(chunks):
        block = got_ref.at[pl.ds(j * group, len(span(j)))]
        pltpu.make_async_copy(block, block, got_sem.at[j]).wait()
        load = pltpu.make_async_copy(got_ref.at[some(j)], rows, load_sem.at[0])
        load.start()
        if j > 0:
            back(j - 1)
        load.wait()
        xs = rows[...].reshape(group * cap, d_model)
        h = jax.nn.gelu(jnp.dot(xs, w1_ref[...], preferred_element_type=F32), approximate=True).astype(BF16)
        z = jnp.dot(h, w2_ref[...], preferred_element_type=F32)
        z = jnp.clip(z, -BF16_MAX, BF16_MAX)
        zv[j % 2] = z.astype(BF16).reshape(group, cap, d_model)
        z_store(j).start()
    back(chunks - 1)
    own_z = pltpu.make_async_copy(zh_ref.at[n - 1], ret_ref.at[n - 1], own_sem)
    own_z.start()
    own_z.wait()

    for j in range(chunks):
        block = ret_ref.at[pl.ds(j * group, len(span(j)))]
        get_hot = pltpu.make_async_copy(hot_hbm.at[j], hot, load_sem.at[1])
        get_hot.start()
        pltpu.make_async_copy(block, block, ret_sem.at[j]).wait()
        load = pltpu.make_async_copy(ret_ref.at[some(j)], rows, load_sem.at[0])
        load.start()
        get_hot.wait()
        load.wait()
        part = jnp.dot(hot[...], rows[...].reshape(group * cap, d_model), preferred_element_type=F32).astype(BF16)
        picked_ref[...] = part if j == 0 else picked_ref[...] + part

    rest = pl.ds(0, n - 1)
    pltpu.make_async_copy(send_ref.at[rest], send_ref.at[rest], out_sem).wait()
    pltpu.make_async_copy(zh_ref.at[rest], zh_ref.at[rest], back_sem).wait()
    pltpu.make_async_copy(all_ref.at[rest], all_ref.at[rest], cnt_out).wait()
    pltpu.make_async_copy(all_ref.at[rest], all_ref.at[rest], cnt_got).wait()


def _finish(capacity, all_ref, x_ref, meta_ref, one_ref, two_ref, out_ref):
    me = lax.axis_index("ep")
    early = lax.broadcasted_iota(I32, all_ref.shape, 0) < me
    base = jnp.sum(jnp.where(early, all_ref[...], 0.0), axis=0)
    meta = meta_ref[...]
    lane = lax.broadcasted_iota(I32, meta.shape, 1).astype(F32)
    y = 0.0
    for k, z_ref in enumerate((one_ref, two_ref)):
        e, pos = meta[:, 2 + k:3 + k], meta[:, 4 + k:5 + k]
        before = pos + jnp.sum(jnp.where(lane == e, base, 0.0), axis=1, keepdims=True)
        y += jnp.where(before < capacity, meta[:, k:k + 1], 0.0) * z_ref[...].astype(F32)
    out_ref[...] = (x_ref[...].astype(F32) + y).astype(BF16)


def solution(mesh):
    n = mesh.shape["ep"]
    row_spec = P(("dp", "ep"), None)
    expert_spec = P("ep", None, None)

    def local_step(x_rows, logits, w_in, w_out):
        tok, d_model = x_rows.shape
        experts = logits.shape[1]
        capacity = CAP_FACTOR * tok * n // experts
        cap = 4 * tok // experts
        group = 16
        chunks, width = n // group, group * cap
        code = np.array([((z * SIDE + y) * SIDE + x) * CORES + c for z, y, x, c in _send_order(n)], np.int32)
        offsets = jnp.asarray(np.repeat(code, cap).reshape(chunks, 1, width))
        whole = lambda *s: pl.BlockSpec(s, lambda i: (0,) * len(s))
        send, hot, meta, cnt = pl.pallas_call(
            functools.partial(_route_pack, n, cap),
            grid=(chunks,),
            in_specs=[whole(tok, experts), whole(tok, d_model), whole(chunks, 1, width)],
            out_specs=[pl.BlockSpec((width, d_model), lambda i: (i, 0)), pl.BlockSpec((2 * tok, width), lambda i: (i, 0)),
                       whole(tok, experts), whole(1, experts)],
            out_shape=[jax.ShapeDtypeStruct((chunks * width, d_model), BF16),
                       jax.ShapeDtypeStruct((chunks * 2 * tok, width), BF16),
                       jax.ShapeDtypeStruct((tok, experts), F32), jax.ShapeDtypeStruct((1, experts), F32)],
            name="route_pack",
        )(logits, x_rows, offsets)

        any_ = pl.BlockSpec(memory_space=pl.ANY)
        vmem = pl.BlockSpec(memory_space=pltpu.VMEM)
        dma = pltpu.SemaphoreType.DMA
        slab = jax.ShapeDtypeStruct((n, cap, d_model), BF16)
        picked, all_cnt = pl.pallas_call(
            functools.partial(_exchange, n, group),
            in_specs=[any_, any_, any_, vmem, vmem],
            out_specs=[vmem, any_, any_, any_, any_],
            out_shape=[jax.ShapeDtypeStruct((2 * tok, d_model), BF16), jax.ShapeDtypeStruct((n, 1, experts), F32),
                       slab, slab, slab],
            scratch_shapes=[pltpu.VMEM((group, cap, d_model), BF16), pltpu.VMEM((2, group, cap, d_model), BF16),
                            pltpu.VMEM((2 * tok, width), BF16),
                            dma, dma((chunks,)), dma, dma((chunks,)), dma, dma, dma, dma((2,)), dma((2,))],
            compiler_params=pltpu.CompilerParams(collective_id=0, has_side_effects=True, vmem_limit_bytes=60 * 2**20),
            name="exchange",
        )(send.reshape(n, cap, d_model), cnt, hot.reshape(chunks, 2 * tok, width), w_in[0], w_out[0])[:2]

        blk = tok // 4
        part = lambda s: pl.BlockSpec((blk, d_model), lambda i: (i + s, 0))
        return pl.pallas_call(
            functools.partial(_finish, capacity),
            grid=(tok // blk,),
            in_specs=[whole(n, 1, experts), part(0), pl.BlockSpec((blk, experts), lambda i: (i, 0)), part(0),
                      part(tok // blk)],
            out_specs=part(0),
            out_shape=jax.ShapeDtypeStruct((tok, d_model), BF16),
            name="finish",
        )(all_cnt, x_rows, meta, picked, picked)

    return jax.shard_map(local_step, mesh=mesh, in_specs=(row_spec, row_spec, expert_spec, expert_spec),
                         out_specs=row_spec, check_vma=False)
```

```python
import functools
import jax
import jax.numpy as jnp
from jax import lax
from jax.experimental import pallas as pl
from jax.experimental.pallas import tpu as pltpu
from jax.sharding import PartitionSpec as P

CAP_FACTOR = 2
HALVES = 2
F32, BF16 = jnp.float32, jnp.bfloat16
MESH = pl.DeviceIdType.MESH
BF16_MAX = float(jnp.finfo(jnp.bfloat16).max)


def _grid_dims(n):
    return n // 32, 4, 4, 2


def _peer(me, n, i, sign):
    p = n - 1
    square = i * i % p
    k = square * square % p * i % p + 1
    nz, ny, nx, nc = _grid_dims(n)
    dz, dy, dx, dc = k // (ny * nx * nc), (k // (nx * nc)) % ny, (k // nc) % nx, k % nc
    if sign < 0:
        dz, dy, dx = nz - dz, ny - dy, nx - dx
    z, y, x, c = me // (ny * nx * nc), (me // (nx * nc)) % ny, (me // nc) % nx, me % nc
    return (((z + dz) % nz * ny + (y + dy) % ny) * nx + (x + dx) % nx) * nc + (c + dc) % nc


def _route_pack(src_cap, logits_ref, x_ref, send_ref, meta_ref, cnt_ref, slot_row):
    step = pl.program_id(0)

    @pl.when(step == 0)
    def _():
        lg = logits_ref[...]
        tok, experts = lg.shape
        lane = lax.broadcasted_iota(jnp.int32, lg.shape, 1)
        m1 = jnp.max(lg, axis=1, keepdims=True)
        i1 = jnp.min(jnp.where(lg == m1, lane, experts), axis=1, keepdims=True)
        rest = jnp.where(lane == i1, -jnp.inf, lg)
        m2 = jnp.max(rest, axis=1, keepdims=True)
        i2 = jnp.min(jnp.where(rest == m2, lane, experts), axis=1, keepdims=True)
        hot1, hot2 = lane == i1, lane == i2
        chosen = jnp.where(hot1 | hot2, 1.0, 0.0)
        total = jnp.sum(jnp.exp(lg - m1), axis=1, keepdims=True)
        g1 = 1.0 / total
        g2 = jnp.exp(m2 - m1) / total
        later = lax.broadcasted_iota(jnp.int32, (tok, tok), 0)
        early = lax.broadcasted_iota(jnp.int32, (tok, tok), 1)
        tri = jnp.where(early < later, 1.0, 0.0).astype(BF16)
        before = jnp.dot(tri, chosen.astype(BF16), preferred_element_type=F32)
        p1 = jnp.sum(jnp.where(hot1, before, 0.0), axis=1, keepdims=True)
        p2 = jnp.sum(jnp.where(hot2, before, 0.0), axis=1, keepdims=True)
        cnt_ref[...] = jnp.sum(chosen, axis=0, keepdims=True)
        e1, e2 = i1.astype(F32), i2.astype(F32)
        part = src_cap // HALVES

        def slot_of(e, p):
            half = jnp.where(p >= part, 1.0, 0.0)
            return half * (experts * part) + e * part + p - half * part

        meta = jnp.where(lane == 0, g1, jnp.where(lane == 1, g2, jnp.where(lane == 2, e1, jnp.where(
            lane == 3, e2, jnp.where(lane == 4, p1, jnp.where(lane == 5, p2, jnp.where(
                lane == 6, slot_of(e1, p1), jnp.where(lane == 7, slot_of(e2, p2), 0.0))))))))
        meta_ref[...] = meta
        slot_row[...] = meta.T[0:8, :].astype(jnp.int32)

    rows = send_ref.shape[0]
    slot = lax.broadcasted_iota(jnp.int32, (rows, x_ref.shape[0]), 0) + step * rows
    pick = (slot == slot_row[6:7, :]) | (slot == slot_row[7:8, :])
    hot = jnp.where(pick, 1.0, 0.0).astype(BF16)
    send_ref[...] = jnp.dot(hot, x_ref[...], preferred_element_type=F32).astype(BF16)


def _exchange(n, group, send_ref, cnt_ref, w1_ref, w2_ref, ret_ref, all_ref, got_ref, zh_ref, rows, zv,
              out_sem, got_sem, back_sem, ret_sem, cnt_out, cnt_got, own_sem, load_sem, store_sem):
    me = lax.axis_index("ep")
    part, d_model = send_ref.shape[2:]
    chunks = n // group

    bar = pltpu.get_barrier_semaphore()

    def greet(k, carry):
        pl.semaphore_signal(bar, inc=1, device_id={"ep": (me + k) % n}, device_id_type=MESH)
        return carry

    lax.fori_loop(1, n, greet, 0)
    pl.semaphore_wait(bar, n - 1)

    def span(c):
        return range(c * group, min((c + 1) * group, n - 1))

    todo = [(h, c) for h in range(HALVES) for c in range(chunks)]
    for j, (h, c) in enumerate(todo):

        def send(i, carry):
            peer = _peer(me, n, i, 1)
            pltpu.make_async_remote_copy(send_ref.at[h, peer], got_ref.at[h, i], out_sem.at[h], got_sem.at[j],
                                         device_id={"ep": peer}, device_id_type=MESH).start()
            return carry

        lax.fori_loop(span(c).start, span(c).stop, send, 0)

    def tell(k, carry):
        pltpu.make_async_remote_copy(cnt_ref, all_ref.at[me], cnt_out, cnt_got, device_id={"ep": (me + k) % n},
                                     device_id_type=MESH).start()
        return carry

    lax.fori_loop(1, n, tell, 0)
    for h in range(HALVES):
        own = pltpu.make_async_copy(send_ref.at[h, me], got_ref.at[h, n - 1], own_sem)
        own.start()
        own.wait()
    own_cnt = pltpu.make_async_copy(cnt_ref, all_ref.at[me], own_sem)
    own_cnt.start()
    own_cnt.wait()

    def z_store(j):
        h, c = todo[j]
        return pltpu.make_async_copy(zv.at[j % 2], zh_ref.at[h, pl.ds(c * group, group)], store_sem.at[j % 2])

    def back(j):
        h, c = todo[j]
        z_store(j).wait()

        def give(i, carry):
            pltpu.make_async_remote_copy(zh_ref.at[h, i], ret_ref.at[h, me], back_sem.at[h], ret_sem.at[h],
                                         device_id={"ep": _peer(me, n, i, -1)}, device_id_type=MESH).start()
            return carry

        lax.fori_loop(span(c).start, span(c).stop, give, 0)

    for j, (h, c) in enumerate(todo):
        block = got_ref.at[h, pl.ds(c * group, len(span(c)))]
        pltpu.make_async_copy(block, block, got_sem.at[j]).wait()
        load = pltpu.make_async_copy(got_ref.at[h, pl.ds(c * group, group)], rows, load_sem)
        load.start()
        if j > 0:
            back(j - 1)
        load.wait()
        xs = rows[...].reshape(group * part, d_model)
        hid = jax.nn.gelu(jnp.dot(xs, w1_ref[...], preferred_element_type=F32), approximate=True).astype(BF16)
        z = jnp.dot(hid, w2_ref[...], preferred_element_type=F32)
        z = jnp.clip(z, -BF16_MAX, BF16_MAX)
        zv[j % 2] = z.astype(BF16).reshape(group, part, d_model)
        z_store(j).start()
    back(len(todo) - 1)
    for h in range(HALVES):
        own_z = pltpu.make_async_copy(zh_ref.at[h, n - 1], ret_ref.at[h, me], own_sem)
        own_z.start()
        own_z.wait()

    rest = pl.ds(0, n - 1)
    for h in range(HALVES):
        pltpu.make_async_copy(send_ref.at[h, rest], send_ref.at[h, rest], out_sem.at[h]).wait()
        pltpu.make_async_copy(zh_ref.at[h, rest], zh_ref.at[h, rest], back_sem.at[h]).wait()
    pltpu.make_async_copy(all_ref.at[rest], all_ref.at[rest], cnt_out).wait()
    pltpu.make_async_copy(all_ref.at[rest], all_ref.at[rest], cnt_got).wait()
    for h in range(HALVES):
        pltpu.make_async_copy(ret_ref.at[h, rest], ret_ref.at[h, rest], ret_sem.at[h]).wait()


def _combine(capacity, all_ref, ret_ref, x_ref, meta_ref, out_ref, pick):
    tok = x_ref.shape[0]

    @pl.when(pl.program_id(0) == 0)
    def _():
        meta = meta_ref[...]
        before_me = lax.broadcasted_iota(jnp.int32, all_ref.shape, 0) < lax.axis_index("ep")
        base = jnp.sum(jnp.where(before_me, all_ref[...], 0.0), axis=0)
        lane = lax.broadcasted_iota(jnp.int32, meta.shape, 1).astype(F32)
        slots = lax.broadcasted_iota(jnp.int32, (tok, pick.shape[1]), 1).astype(F32)
        for c in range(2):
            e, pos, slot = meta[:, 2 + c:3 + c], meta[:, 4 + c:5 + c], meta[:, 6 + c:7 + c]
            ahead = jnp.sum(jnp.where(lane == e, base, 0.0), axis=1, keepdims=True)
            slot = jnp.where(pos + ahead < capacity, slot, -1.0)
            pick[c * tok:(c + 1) * tok, :] = jnp.where(slots == slot, 1.0, 0.0).astype(BF16)

    z = ret_ref[...]
    z = jnp.where(z == z, z, jnp.zeros_like(z))
    r = jnp.dot(pick[...], z, preferred_element_type=F32)
    y = meta_ref[:, 0:1] * r[0:tok] + meta_ref[:, 1:2] * r[tok:2 * tok]
    out_ref[...] = (x_ref[...].astype(F32) + y).astype(BF16)


def solution(mesh):
    n = mesh.shape["ep"]
    row_spec = P(("dp", "ep"), None)
    expert_spec = P("ep", None, None)

    def local_step(x_rows, logits, w_in, w_out):
        tok, d_model = x_rows.shape
        experts = logits.shape[1]
        ff = w_in.shape[2]
        capacity = CAP_FACTOR * tok * n // experts
        src_cap = 4 * tok // experts
        slots = experts * src_cap
        blk = 256
        whole = lambda *s: pl.BlockSpec(s, lambda i: (0,) * len(s))
        send, meta, cnt = pl.pallas_call(
            functools.partial(_route_pack, src_cap),
            grid=(slots // blk,),
            in_specs=[whole(tok, experts), whole(tok, d_model)],
            out_specs=[pl.BlockSpec((blk, d_model), lambda i: (i, 0)), whole(tok, experts), whole(1, experts)],
            out_shape=[jax.ShapeDtypeStruct((slots, d_model), BF16), jax.ShapeDtypeStruct((tok, experts), F32),
                       jax.ShapeDtypeStruct((1, experts), F32)],
            scratch_shapes=[pltpu.VMEM((8, tok), jnp.int32)],
            name="route_pack",
        )(logits, x_rows)

        group = 32
        part = src_cap // HALVES
        slab = jax.ShapeDtypeStruct((HALVES, n, part, d_model), BF16)
        any_ = pl.BlockSpec(memory_space=pl.ANY)
        vmem = pl.BlockSpec(memory_space=pltpu.VMEM)
        dma = pltpu.SemaphoreType.DMA
        ret, all_cnt, _, _ = pl.pallas_call(
            functools.partial(_exchange, n, group),
            in_specs=[any_, any_, vmem, vmem],
            out_specs=[any_, any_, any_, any_],
            out_shape=[slab, jax.ShapeDtypeStruct((n, 1, experts), F32),
                       slab,
                       slab],
            scratch_shapes=[pltpu.VMEM((group, part, d_model), BF16), pltpu.VMEM((2, group, part, d_model), BF16),
                            dma((HALVES,)), dma((HALVES * n // group,)), dma((HALVES,)), dma((HALVES,)), dma, dma, dma, dma, dma((2,))],
            compiler_params=pltpu.CompilerParams(collective_id=0, has_side_effects=True, vmem_limit_bytes=60 * 2**20),
            name="exchange",
        )(send.reshape(HALVES, n, part, d_model), cnt, w_in[0], w_out[0])

        cols = 256
        return pl.pallas_call(
            functools.partial(_combine, capacity),
            grid=(d_model // cols,),
            in_specs=[whole(n, 1, experts), pl.BlockSpec((slots, cols), lambda i: (0, i)),
                      pl.BlockSpec((tok, cols), lambda i: (0, i)), whole(tok, experts)],
            out_specs=pl.BlockSpec((tok, cols), lambda i: (0, i)),
            out_shape=jax.ShapeDtypeStruct((tok, d_model), BF16),
            scratch_shapes=[pltpu.VMEM((2 * tok, slots), BF16)],
            name="combine",
        )(all_cnt, ret.reshape(slots, d_model), x_rows, meta)

    return jax.shard_map(local_step, mesh=mesh, in_specs=(row_spec, row_spec, expert_spec, expert_spec),
                         out_specs=row_spec, check_vma=False)
```

```python
import functools
import jax
import jax.numpy as jnp
from jax import lax
from jax.experimental import pallas as pl
from jax.experimental.pallas import tpu as pltpu
from jax.sharding import PartitionSpec as P

CAP_FACTOR = 2
HALVES = 2
F32, BF16 = jnp.float32, jnp.bfloat16
MESH = pl.DeviceIdType.MESH
BF16_MAX = float(jnp.finfo(jnp.bfloat16).max)


def _grid_dims(n):
    return n // 32, 4, 4, 2


def _peer(me, n, i, sign):
    p = n - 1
    square = i * i % p
    k = square * square % p * i % p + 1
    nz, ny, nx, nc = _grid_dims(n)
    dz, dy, dx, dc = k // (ny * nx * nc), (k // (nx * nc)) % ny, (k // nc) % nx, k % nc
    if sign < 0:
        dz, dy, dx = nz - dz, ny - dy, nx - dx
    z, y, x, c = me // (ny * nx * nc), (me // (nx * nc)) % ny, (me // nc) % nx, me % nc
    return (((z + dz) % nz * ny + (y + dy) % ny) * nx + (x + dx) % nx) * nc + (c + dc) % nc


def _route(src_cap, logits_ref, pick_ref, meta_ref, cnt_ref, slot_row):
    step = pl.program_id(0)

    @pl.when(step == 0)
    def _():
        lg = logits_ref[...]
        tok, experts = lg.shape
        lane = lax.broadcasted_iota(jnp.int32, lg.shape, 1)
        m1 = jnp.max(lg, axis=1, keepdims=True)
        i1 = jnp.min(jnp.where(lg == m1, lane, experts), axis=1, keepdims=True)
        rest = jnp.where(lane == i1, -jnp.inf, lg)
        m2 = jnp.max(rest, axis=1, keepdims=True)
        i2 = jnp.min(jnp.where(rest == m2, lane, experts), axis=1, keepdims=True)
        hot1, hot2 = lane == i1, lane == i2
        chosen = jnp.where(hot1 | hot2, 1.0, 0.0)
        total = jnp.sum(jnp.exp(lg - m1), axis=1, keepdims=True)
        g1 = 1.0 / total
        g2 = jnp.exp(m2 - m1) / total
        later = lax.broadcasted_iota(jnp.int32, (tok, tok), 0)
        early = lax.broadcasted_iota(jnp.int32, (tok, tok), 1)
        tri = jnp.where(early < later, 1.0, 0.0).astype(BF16)
        before = jnp.dot(tri, chosen.astype(BF16), preferred_element_type=F32)
        p1 = jnp.sum(jnp.where(hot1, before, 0.0), axis=1, keepdims=True)
        p2 = jnp.sum(jnp.where(hot2, before, 0.0), axis=1, keepdims=True)
        cnt_ref[...] = jnp.sum(chosen, axis=0, keepdims=True)
        e1, e2 = i1.astype(F32), i2.astype(F32)
        part = src_cap // HALVES

        def slot_of(e, p):
            half = jnp.where(p >= part, 1.0, 0.0)
            return half * (experts * part) + e * part + p - half * part

        meta = jnp.where(lane == 0, g1, jnp.where(lane == 1, g2, jnp.where(lane == 2, e1, jnp.where(
            lane == 3, e2, jnp.where(lane == 4, p1, jnp.where(lane == 5, p2, jnp.where(
                lane == 6, slot_of(e1, p1), jnp.where(lane == 7, slot_of(e2, p2), 0.0))))))))
        meta_ref[...] = meta
        slot_row[...] = meta.T[0:8, :].astype(jnp.int32)

    rows, tok = pick_ref.shape
    slot = lax.broadcasted_iota(jnp.int32, (rows, tok), 0) + step * rows
    pick = (slot == slot_row[6:7, :]) | (slot == slot_row[7:8, :])
    pick_ref[...] = jnp.where(pick, 1.0, 0.0).astype(BF16)


def _exchange(n, group, pick_ref, x_ref, cnt_ref, w1_ref, w2_ref, ret_ref, all_ref, send_ref, got_ref, zh_ref, rows, zv,
              out_sem, got_sem, back_sem, ret_sem, cnt_out, cnt_got, own_sem, load_sem, store_sem):
    me = lax.axis_index("ep")
    part, d_model = send_ref.shape[2:]
    chunks = n // group

    bar = pltpu.get_barrier_semaphore()

    def greet(k, carry):
        pl.semaphore_signal(bar, inc=1, device_id={"ep": (me + k) % n}, device_id_type=MESH)
        return carry

    lax.fori_loop(1, n, greet, 0)

    def span(c):
        return range(c * group, min((c + 1) * group, n - 1))

    todo = [(h, c) for h in range(HALVES) for c in range(chunks)]

    def pack(j):
        h, c = todo[j]
        return pltpu.make_async_copy(zv.at[j % 2], send_ref.at[h, pl.ds(c * group, group)], store_sem.at[j % 2])

    width = group * part
    for j, (h, c) in enumerate(todo):
        if c >= 2:
            pack(j - 2).wait()
        rows_now = jnp.dot(pick_ref[j * width:(j + 1) * width, :], x_ref[...], preferred_element_type=F32)
        zv[j % 2] = rows_now.astype(BF16).reshape(group, part, d_model)
        pack(j).start()
        if c < chunks - 1:
            continue
        if h == 0:
            pl.semaphore_wait(bar, n - 1)
        pack(j - 1).wait()
        pack(j).wait()

        def send(at, i, carry, h=h):
            peer = _peer(me, n, i, 1)
            pltpu.make_async_remote_copy(send_ref.at[h, peer], got_ref.at[h, i], out_sem.at[h], got_sem.at[at],
                                         device_id={"ep": peer}, device_id_type=MESH).start()
            return carry

        for k in range(chunks):
            lax.fori_loop(span(k).start, span(k).stop, functools.partial(send, h * chunks + k), 0)

    def tell(k, carry):
        pltpu.make_async_remote_copy(cnt_ref, all_ref.at[me], cnt_out, cnt_got, device_id={"ep": (me + k) % n},
                                     device_id_type=MESH).start()
        return carry

    lax.fori_loop(1, n, tell, 0)
    for h in range(HALVES):
        own = pltpu.make_async_copy(send_ref.at[h, me], got_ref.at[h, n - 1], own_sem)
        own.start()
        own.wait()
    own_cnt = pltpu.make_async_copy(cnt_ref, all_ref.at[me], own_sem)
    own_cnt.start()
    own_cnt.wait()

    def z_store(j):
        h, c = todo[j]
        return pltpu.make_async_copy(zv.at[j % 2], zh_ref.at[h, pl.ds(c * group, group)], store_sem.at[j % 2])

    def back(j):
        h, c = todo[j]
        z_store(j).wait()

        def give(i, carry):
            pltpu.make_async_remote_copy(zh_ref.at[h, i], ret_ref.at[h, me], back_sem.at[h], ret_sem.at[h],
                                         device_id={"ep": _peer(me, n, i, -1)}, device_id_type=MESH).start()
            return carry

        lax.fori_loop(span(c).start, span(c).stop, give, 0)

    for j, (h, c) in enumerate(todo):
        block = got_ref.at[h, pl.ds(c * group, len(span(c)))]
        pltpu.make_async_copy(block, block, got_sem.at[j]).wait()
        load = pltpu.make_async_copy(got_ref.at[h, pl.ds(c * group, group)], rows, load_sem)
        load.start()
        if j > 0:
            back(j - 1)
        load.wait()
        xs = rows[...].reshape(group * part, d_model)
        hid = jax.nn.gelu(jnp.dot(xs, w1_ref[...], preferred_element_type=F32), approximate=True).astype(BF16)
        z = jnp.dot(hid, w2_ref[...], preferred_element_type=F32)
        z = jnp.clip(z, -BF16_MAX, BF16_MAX)
        zv[j % 2] = z.astype(BF16).reshape(group, part, d_model)
        z_store(j).start()
    back(len(todo) - 1)
    for h in range(HALVES):
        own_z = pltpu.make_async_copy(zh_ref.at[h, n - 1], ret_ref.at[h, me], own_sem)
        own_z.start()
        own_z.wait()

    rest = pl.ds(0, n - 1)
    for h in range(HALVES):
        pltpu.make_async_copy(send_ref.at[h, rest], send_ref.at[h, rest], out_sem.at[h]).wait()
        pltpu.make_async_copy(zh_ref.at[h, rest], zh_ref.at[h, rest], back_sem.at[h]).wait()
    pltpu.make_async_copy(all_ref.at[rest], all_ref.at[rest], cnt_out).wait()
    pltpu.make_async_copy(all_ref.at[rest], all_ref.at[rest], cnt_got).wait()
    for h in range(HALVES):
        pltpu.make_async_copy(ret_ref.at[h, rest], ret_ref.at[h, rest], ret_sem.at[h]).wait()


def _combine(capacity, all_ref, ret_ref, x_ref, meta_ref, out_ref, pick):
    tok = x_ref.shape[0]

    @pl.when(pl.program_id(0) == 0)
    def _():
        meta = meta_ref[...]
        before_me = lax.broadcasted_iota(jnp.int32, all_ref.shape, 0) < lax.axis_index("ep")
        base = jnp.sum(jnp.where(before_me, all_ref[...], 0.0), axis=0)
        lane = lax.broadcasted_iota(jnp.int32, meta.shape, 1).astype(F32)
        slots = lax.broadcasted_iota(jnp.int32, (tok, pick.shape[1]), 1).astype(F32)
        for c in range(2):
            e, pos, slot = meta[:, 2 + c:3 + c], meta[:, 4 + c:5 + c], meta[:, 6 + c:7 + c]
            ahead = jnp.sum(jnp.where(lane == e, base, 0.0), axis=1, keepdims=True)
            slot = jnp.where(pos + ahead < capacity, slot, -1.0)
            pick[c * tok:(c + 1) * tok, :] = jnp.where(slots == slot, 1.0, 0.0).astype(BF16)

    z = ret_ref[...]
    z = jnp.where(z == z, z, jnp.zeros_like(z))
    r = jnp.dot(pick[...], z, preferred_element_type=F32)
    y = meta_ref[:, 0:1] * r[0:tok] + meta_ref[:, 1:2] * r[tok:2 * tok]
    out_ref[...] = (x_ref[...].astype(F32) + y).astype(BF16)


def solution(mesh):
    n = mesh.shape["ep"]
    row_spec = P(("dp", "ep"), None)
    expert_spec = P("ep", None, None)

    def local_step(x_rows, logits, w_in, w_out):
        tok, d_model = x_rows.shape
        experts = logits.shape[1]
        ff = w_in.shape[2]
        capacity = CAP_FACTOR * tok * n // experts
        src_cap = 4 * tok // experts
        slots = experts * src_cap
        blk = 256
        whole = lambda *s: pl.BlockSpec(s, lambda i: (0,) * len(s))
        pick, meta, cnt = pl.pallas_call(
            functools.partial(_route, src_cap),
            grid=(slots // blk,),
            in_specs=[whole(tok, experts)],
            out_specs=[pl.BlockSpec((blk, tok), lambda i: (i, 0)), whole(tok, experts), whole(1, experts)],
            out_shape=[jax.ShapeDtypeStruct((slots, tok), BF16), jax.ShapeDtypeStruct((tok, experts), F32),
                       jax.ShapeDtypeStruct((1, experts), F32)],
            scratch_shapes=[pltpu.VMEM((8, tok), jnp.int32)],
            name="route",
        )(logits)

        group = 32
        part = src_cap // HALVES
        slab = jax.ShapeDtypeStruct((HALVES, n, part, d_model), BF16)
        any_ = pl.BlockSpec(memory_space=pl.ANY)
        vmem = pl.BlockSpec(memory_space=pltpu.VMEM)
        dma = pltpu.SemaphoreType.DMA
        ret, all_cnt = pl.pallas_call(
            functools.partial(_exchange, n, group),
            in_specs=[vmem, vmem, any_, vmem, vmem],
            out_specs=[any_, any_, any_, any_, any_],
            out_shape=[slab, jax.ShapeDtypeStruct((n, 1, experts), F32),
                       slab,
                       slab, slab],
            scratch_shapes=[pltpu.VMEM((group, part, d_model), BF16), pltpu.VMEM((2, group, part, d_model), BF16),
                            dma((HALVES,)), dma((HALVES * n // group,)), dma((HALVES,)), dma((HALVES,)), dma, dma, dma, dma, dma((2,))],
            compiler_params=pltpu.CompilerParams(collective_id=0, has_side_effects=True, vmem_limit_bytes=60 * 2**20),
            name="exchange",
        )(pick, x_rows, cnt, w_in[0], w_out[0])[:2]

        cols = 256
        return pl.pallas_call(
            functools.partial(_combine, capacity),
            grid=(d_model // cols,),
            in_specs=[whole(n, 1, experts), pl.BlockSpec((slots, cols), lambda i: (0, i)),
                      pl.BlockSpec((tok, cols), lambda i: (0, i)), whole(tok, experts)],
            out_specs=pl.BlockSpec((tok, cols), lambda i: (0, i)),
            out_shape=jax.ShapeDtypeStruct((tok, d_model), BF16),
            scratch_shapes=[pltpu.VMEM((2 * tok, slots), BF16)],
            name="combine",
        )(all_cnt, ret.reshape(slots, d_model), x_rows, meta)

    return jax.shard_map(local_step, mesh=mesh, in_specs=(row_spec, row_spec, expert_spec, expert_spec),
                         out_specs=row_spec, check_vma=False)
```
